64 devices in a mesh: dp: 4 (over x, y), tp: 16 (over z, core).
Axes of the slice: x: 2, y: 2, z: 8, core: 2. Of those that a mesh axis runs over, the one named last changes fastest.
The devices are a block of a 4x4x8 slice.
Arguments:
- hidden: bfloat16 [4, 4096, 3072], P('dp', 'tp'), parts along dimension 0
- ln1_gain: float32 [3072], replicated
- ln1_bias: float32 [3072], replicated
- w_qkv: bfloat16 [3072, 3, 32, 96], P(None, None, 'tp')
- b_qkv: bfloat16 [3, 32, 96], P(None, 'tp')
- w_out: bfloat16 [32, 96, 3072], P('tp')
- b_out: bfloat16 [3072], replicated
- ln2_gain: float32 [3072], replicated
- ln2_bias: float32 [3072], replicated
- w_up: bfloat16 [3072, 12288], P(None, 'tp')
- b_up: bfloat16 [12288], P('tp')
- w_down: bfloat16 [12288, 3072], P('tp')
- b_down: bfloat16 [3072], replicated
Outputs:
- output: bfloat16 [4, 4096, 3072], P('dp', 'tp'), parts along dimension 0
There are 4 independent parts. The reference program is written for one: setup_inputs(seed, part) draws one part's arguments, and reference() takes and returns one part's arrays. A program takes and returns all parts, laid end to end along the dimension named above; an argument that names none is the same for every part.
All inputs are finite; a program needn't handle non-finite values.
Results may differ from the reference program's by a relative error of at most 0.0105452.
Values are sent between devices in bfloat16 or wider.
A program may use at most 768 MiB of HBM per device.

```python
import math
import jax
import jax.numpy as jnp
from jax import lax

N_BATCH = 1
SEQ_LEN = 4096
D_MODEL = 3072
N_HEADS = 32

HEAD_DIM = D_MODEL // N_HEADS
FF_DIM = 4 * D_MODEL
LN_EPS = 1e-5


def layer_norm(inputs, gain_vec, shift_vec):
    as_f32 = inputs.astype(jnp.float32)
    row_mean = jnp.mean(as_f32, axis=-1, keepdims=True)
    centered = as_f32 - row_mean
    variance = jnp.mean(centered * centered, axis=-1, keepdims=True)
    return (centered * lax.rsqrt(variance + LN_EPS) * gain_vec + shift_vec).astype(jnp.bfloat16)


def setup_inputs(seed: int = 0, part: int = 0) -> dict:
    root_key = jax.random.key(seed)
    sub_keys = jax.random.split(root_key, 13)
    qk_gain = (0.5 * math.log(SEQ_LEN)) ** 0.25
    col_gain = jnp.array([qk_gain, qk_gain, 1.0], jnp.float32).reshape(1, 3, 1, 1)
    hidden = jax.random.normal(jax.random.fold_in(sub_keys[0], part), (N_BATCH, SEQ_LEN, D_MODEL), jnp.float32)
    w_qkv = jax.random.normal(sub_keys[3], (D_MODEL, 3, N_HEADS, HEAD_DIM), jnp.float32) * col_gain * D_MODEL ** -0.5
    return {
        "hidden": hidden.astype(jnp.bfloat16),
        "ln1_gain": 1.0 + 0.3 * jax.random.normal(sub_keys[1], (D_MODEL,), jnp.float32),
        "ln1_bias": 0.3 * jax.random.normal(sub_keys[2], (D_MODEL,), jnp.float32),
        "w_qkv": w_qkv.astype(jnp.bfloat16),
        "b_qkv": (0.5 * jax.random.normal(sub_keys[4], (3, N_HEADS, HEAD_DIM), jnp.float32)).astype(jnp.bfloat16),
        "w_out": (jax.random.normal(sub_keys[5], (N_HEADS, HEAD_DIM, D_MODEL), jnp.float32) * D_MODEL ** -0.5).astype(jnp.bfloat16),
        "b_out": (0.3 * jax.random.normal(sub_keys[6], (D_MODEL,), jnp.float32)).astype(jnp.bfloat16),
        "ln2_gain": 1.0 + 0.3 * jax.random.normal(sub_keys[7], (D_MODEL,), jnp.float32),
        "ln2_bias": 0.3 * jax.random.normal(sub_keys[8], (D_MODEL,), jnp.float32),
        "w_up": (jax.random.normal(sub_keys[9], (D_MODEL, FF_DIM), jnp.float32) * D_MODEL ** -0.5).astype(jnp.bfloat16),
        "b_up": (0.5 * jax.random.normal(sub_keys[10], (FF_DIM,), jnp.float32)).astype(jnp.bfloat16),
        "w_down": (jax.random.normal(sub_keys[11], (FF_DIM, D_MODEL), jnp.float32) * FF_DIM ** -0.5).astype(jnp.bfloat16),
        "b_down": (0.3 * jax.random.normal(sub_keys[12], (D_MODEL,), jnp.float32)).astype(jnp.bfloat16),
    }


def reference(hidden, ln1_gain, ln1_bias, w_qkv, b_qkv, w_out, b_out, ln2_gain, ln2_bias, w_up, b_up, w_down, b_down):
    normed = layer_norm(hidden, ln1_gain, ln1_bias).reshape(N_BATCH * SEQ_LEN, D_MODEL)
    qkv_acc = jnp.dot(normed, w_qkv.reshape(D_MODEL, 3 * D_MODEL), preferred_element_type=jnp.float32)
    qkv_all = (qkv_acc + b_qkv.reshape(3 * D_MODEL).astype(jnp.float32)).astype(jnp.bfloat16)
    head_major = jnp.transpose(qkv_all.reshape(N_BATCH, SEQ_LEN, 3, N_HEADS, HEAD_DIM), (2, 3, 0, 1, 4))
    positions = jnp.arange(SEQ_LEN)
    causal = positions[:, None] >= positions[None, :]

    def one_head(operands):
        queries, keys_all, values = operands
        logits = jnp.einsum("bqd,bkd->bqk", queries.astype(jnp.float32), keys_all.astype(jnp.float32)) * HEAD_DIM ** -0.5
        logits = jnp.where(causal, logits, -1e30)
        row_max = jnp.max(logits, axis=-1, keepdims=True)
        exp_vals = jnp.exp(logits - row_max)
        weights_bf = (exp_vals / jnp.sum(exp_vals, axis=-1, keepdims=True)).astype(jnp.bfloat16)
        return jnp.einsum("bqk,bkd->bqd", weights_bf.astype(jnp.float32), values.astype(jnp.float32)).astype(jnp.bfloat16)

    context = lax.map(one_head, (head_major[0], head_major[1], head_major[2]))
    attn_sum = jnp.einsum("hbsd,hde->bse", context.astype(jnp.float32), w_out.astype(jnp.float32))
    resid_mid = (hidden.astype(jnp.float32) + (attn_sum + b_out.astype(jnp.float32))).astype(jnp.bfloat16)
    normed_mid = layer_norm(resid_mid, ln2_gain, ln2_bias).reshape(N_BATCH * SEQ_LEN, D_MODEL)
    up_proj = jnp.dot(normed_mid, w_up, preferred_element_type=jnp.float32) + b_up.astype(jnp.float32)
    gelu_out = jax.nn.gelu(up_proj, approximate=True).astype(jnp.bfloat16)
    down_sum = jnp.dot(gelu_out, w_down, preferred_element_type=jnp.float32) + b_down.astype(jnp.float32)
    return (resid_mid.astype(jnp.float32) + down_sum.reshape(N_BATCH, SEQ_LEN, D_MODEL)).astype(jnp.bfloat16)
```

```python
import functools
import math

import jax
import jax.numpy as jnp
from jax import lax
from jax.experimental import pallas as pl
from jax.experimental.pallas import tpu as pltpu
from jax.sharding import PartitionSpec as P

LN_EPS = 1e-5
LANES = 128
MESH_IDS = pl.DeviceIdType.MESH


def layer_norm(inputs, gain_vec, shift_vec):
    as_f32 = inputs.astype(jnp.float32)
    row_mean = jnp.mean(as_f32, axis=-1, keepdims=True)
    centered = as_f32 - row_mean
    variance = jnp.mean(centered * centered, axis=-1, keepdims=True)
    return (centered * lax.rsqrt(variance + LN_EPS) * gain_vec + shift_vec).astype(jnp.bfloat16)


def attention_kernel(blk, scale, q_ref, k_ref, v_ref, o_ref):
    n_heads, seq, width = q_ref.shape
    factor = scale * math.log2(math.e)
    row = lax.broadcasted_iota(jnp.int32, (blk, blk), 0)
    col = lax.broadcasted_iota(jnp.int32, (blk, blk), 1)

    def block(queries, j, carry, masked):
        out = []
        for h in range(n_heads):
            m, l, acc = carry[h]
            rows = pl.ds(pl.multiple_of(j * blk, blk), blk)
            s = lax.dot_general(queries[h], k_ref[h, rows, :], (((1,), (1,)), ((), ())),
                                preferred_element_type=jnp.float32)
            if masked:
                s = jnp.where(row >= col, s, -1e30)
            m_new = jnp.maximum(m, jnp.max(s, axis=-1, keepdims=True))
            p = jnp.exp2((s - m_new) * factor)
            alpha = jnp.exp2((m - m_new) * factor)
            l = l * alpha + jnp.sum(p, axis=-1, keepdims=True)
            acc = acc * alpha + jnp.dot(p.astype(jnp.bfloat16), v_ref[h, rows, :],
                                        preferred_element_type=jnp.float32)
            out.append((m_new, l, acc))
        return tuple(out)

    def per_block(i, _):
        rows = pl.ds(pl.multiple_of(i * blk, blk), blk)
        queries = [q_ref[h, rows, :] for h in range(n_heads)]
        init = tuple(
            (jnp.full((blk, 1), -1e30, jnp.float32), jnp.zeros((blk, 1), jnp.float32),
             jnp.zeros((blk, width), jnp.float32)) for _ in range(n_heads))
        carry = block(queries, i, init, True)
        carry = lax.fori_loop(0, i, lambda j, c: block(queries, j, c, False), carry)
        for h in range(n_heads):
            o_ref[h, rows, :] = (carry[h][2] / carry[h][1]).astype(o_ref.dtype)
        return 0

    lax.fori_loop(0, seq // blk, per_block, 0)


def attention(q, k, v, head_dim):
    n_heads, seq, width = q.shape
    blk = min(512, seq)
    return pl.pallas_call(
        functools.partial(attention_kernel, blk, head_dim ** -0.5),
        out_shape=jax.ShapeDtypeStruct((n_heads, seq, width), jnp.bfloat16),
        in_specs=[pl.BlockSpec(memory_space=pltpu.VMEM)] * 3,
        out_specs=pl.BlockSpec(memory_space=pltpu.VMEM),
        compiler_params=pltpu.CompilerParams(vmem_limit_bytes=48 * 2 ** 20),
        cost_estimate=pl.CostEstimate(flops=4 * n_heads * seq * seq * width, bytes_accessed=8 * n_heads * seq * width,
                                      transcendentals=n_heads * seq * seq // 2),
        name="attention",
    )(q, k, v)


def neighbours(tp):
    me = lax.axis_index("tp")
    core = lax.rem(me, 2)
    right = lax.rem(me + 2, tp)
    left = lax.rem(me + tp - 2, tp)
    sibling = me + 1 - 2 * core
    return right, left, sibling


def entry_barrier(peers):
    barrier = pltpu.get_barrier_semaphore()
    for peer in peers:
        pl.semaphore_signal(barrier, inc=1, device_id={"tp": peer}, device_id_type=MESH_IDS)
    pl.semaphore_wait(barrier, len(peers))


def remote(src, dst, send_sem, recv_sem, peer):
    return pltpu.make_async_remote_copy(src_ref=src, dst_ref=dst, send_sem=send_sem, recv_sem=recv_sem,
                                        device_id={"tp": peer}, device_id_type=MESH_IDS)


def mlp_kernel(tp, up_tile, down_tile, h_hbm, x_ref, wu_hbm, bu_ref, wd_hbm, bd_ref, out_ref,
               ag, part, rs, wu, wd, u_ref, load_sem, ag_send, ag_recv, push_send, push_recv,
               part_send, part_recv, rs_send, rs_recv):
    n = tp // 2
    half = ag.shape[3]
    d_model = ag.shape[4]
    ff = wu.shape[1]
    right, left, sibling = neighbours(tp)
    ahead = (right, left)

    loads = [pltpu.make_async_copy(h_hbm.at[pl.ds(d * half, half)], ag.at[0, d, 0], load_sem.at[d]) for d in range(2)]
    loads.append(pltpu.make_async_copy(wu_hbm, wu, load_sem.at[2]))
    loads.append(pltpu.make_async_copy(wd_hbm, wd, load_sem.at[3]))
    for copy in loads:
        copy.start()
    entry_barrier((right, left, sibling))

    def forward(s, d):
        return remote(ag.at[s, d, 0], ag.at[s + 1, d, 0], ag_send.at[s, d], ag_recv.at[s + 1, d], ahead[d])

    def push(s, d):
        return remote(ag.at[s, d, 0], ag.at[s, d, 1], push_send.at[s, d], push_recv.at[s, d], sibling)

    def give(s, d):
        return remote(ag.at[s, d, 1], part.at[s, d], part_send.at[s, d], part_recv.at[s, d], sibling)

    def reduce_send(s, d):
        return remote(part.at[s, d], rs.at[s, d], rs_send.at[s, d], rs_recv.at[s, d], ahead[d])

    for d in range(2):
        loads[d].wait()
        forward(0, d).start()
        push(0, d).start()
    loads[2].wait()
    loads[3].wait()

    def stage(i, _):
        s = lax.rem(i, n)
        last = i == n

        for d in range(2):
            @pl.when(jnp.logical_not(last))
            def _():
                forward(s - 1, d).wait_recv()

                @pl.when(i < n - 1)
                def _():
                    forward(s, d).start()

                push(s, d).start()

        for d in range(2):
            push(s, d).wait_recv()

        def up(t, _):
            cols = pl.ds(pl.multiple_of(t * up_tile, up_tile), up_tile)
            acc = jnp.dot(ag[s].reshape(4 * half, d_model), wu[:, cols], preferred_element_type=jnp.float32)
            u_ref[:, cols] = jax.nn.gelu(acc + bu_ref[:, cols].astype(jnp.float32), approximate=True).astype(jnp.bfloat16)
            return 0

        lax.fori_loop(0, ff // up_tile, up, 0)

        def down_sibling(t, _):
            cols = pl.ds(pl.multiple_of(t * down_tile, down_tile), down_tile)
            lhs = jnp.concatenate([u_ref[pl.ds(half, half), :], u_ref[pl.ds(3 * half, half), :]], axis=0)
            acc = jnp.dot(lhs, wd[:, cols], preferred_element_type=jnp.float32)
            for d in range(2):
                ag[s, d, 1, :, cols] = acc[d * half:(d + 1) * half].astype(jnp.bfloat16)
            return 0

        lax.fori_loop(0, d_model // down_tile, down_sibling, 0)
        for d in range(2):
            give(s, d).start()
        for d in range(2):
            give(s, d).wait_recv()

            @pl.when(i >= 2)
            def _():
                reduce_send(i - 1, d).wait_recv()

        def own_rows(t):
            cols = pl.ds(pl.multiple_of(t * down_tile, down_tile), down_tile)
            lhs = jnp.concatenate([u_ref[pl.ds(0, half), :], u_ref[pl.ds(2 * half, half), :]], axis=0)
            return cols, jnp.dot(lhs, wd[:, cols], preferred_element_type=jnp.float32)

        def add_terms(acc, d, cols, first):
            total = acc[d * half:(d + 1) * half] + part[s, d, :, cols].astype(jnp.float32)
            return total if first else total + rs[i - 1, d, :, cols].astype(jnp.float32)

        def down_first(t, _):
            cols, acc = own_rows(t)
            for d in range(2):
                part[s, d, :, cols] = add_terms(acc, d, cols, True).astype(jnp.bfloat16)
            return 0

        def down_middle(t, _):
            cols, acc = own_rows(t)
            for d in range(2):
                part[s, d, :, cols] = add_terms(acc, d, cols, False).astype(jnp.bfloat16)
            return 0

        def down_last(t, _):
            cols, acc = own_rows(t)
            bias = bd_ref[:, cols].astype(jnp.float32)
            for d in range(2):
                rows = pl.ds(d * half, half)
                total = add_terms(acc, d, cols, False) + bias
                out_ref[rows, cols] = (x_ref[rows, cols].astype(jnp.float32) + total).astype(jnp.bfloat16)
            return 0

        tiles = d_model // down_tile

        @pl.when(i == 1)
        def _():
            lax.fori_loop(0, tiles, down_first, 0)

        @pl.when(jnp.logical_and(i > 1, i < n))
        def _():
            lax.fori_loop(0, tiles, down_middle, 0)

        @pl.when(i < n)
        def _():
            for d in range(2):
                reduce_send(s, d).start()

        @pl.when(last)
        def _():
            lax.fori_loop(0, tiles, down_last, 0)

        return 0

    lax.fori_loop(1, n + 1, stage, 0)

    def drain(s, _):
        for d in range(2):
            push(s, d).wait_send()
            give(s, d).wait_send()

            @pl.when(s < n - 1)
            def _():
                forward(s, d).wait_send()

            @pl.when(s >= 1)
            def _():
                reduce_send(s, d).wait_send()
        return 0

    lax.fori_loop(0, n, drain, 0)


def mlp(tp, h, x, w_up, b_up, w_down, b_down):
    rows, d_model = h.shape
    ff = w_up.shape[1]
    n, half = tp // 2, rows // 2
    up_tile, down_tile = min(256, ff), min(512, d_model)
    vmem = pl.BlockSpec(memory_space=pltpu.VMEM)
    hbm = pl.BlockSpec(memory_space=pl.ANY)
    dma = pltpu.SemaphoreType.DMA
    return pl.pallas_call(
        functools.partial(mlp_kernel, tp, up_tile, down_tile),
        out_shape=jax.ShapeDtypeStruct((rows, d_model), jnp.bfloat16),
        in_specs=[hbm, vmem, hbm, vmem, hbm, vmem],
        out_specs=vmem,
        scratch_shapes=[
            pltpu.VMEM((n, 2, 2, half, d_model), jnp.bfloat16),
            pltpu.VMEM((n, 2, half, d_model), jnp.bfloat16),
            pltpu.VMEM((n, 2, half, d_model), jnp.bfloat16),
            pltpu.VMEM((d_model, ff), jnp.bfloat16),
            pltpu.VMEM((ff, d_model), jnp.bfloat16),
            pltpu.VMEM((4 * half, ff), jnp.bfloat16),
            dma((4,)),
        ] + [dma((n, 2))] * 8,
        compiler_params=pltpu.CompilerParams(collective_id=1, has_side_effects=True, vmem_limit_bytes=67043328),
        cost_estimate=pl.CostEstimate(flops=4 * tp * rows * d_model * ff, bytes_accessed=4 * d_model * ff, transcendentals=tp * rows * ff),
        name="mlp",
    )(h, x, w_up, b_up.reshape(1, ff), w_down, b_down.reshape(1, d_model))


def solution(mesh):
    tp = mesh.shape["tp"]

    def device_body(hidden, ln1_gain, ln1_bias, w_qkv, b_qkv, w_out, b_out, ln2_gain, ln2_bias, w_up, b_up, w_down, b_down):
        rows, d_model = hidden.shape[1], hidden.shape[2]
        n_heads, head_dim = w_qkv.shape[2], w_qkv.shape[3]
        x = hidden[0]
        normed = layer_norm(x, ln1_gain, ln1_bias)
        normed_all = lax.all_gather(normed, "tp", axis=0, tiled=True)
        pad = LANES - head_dim
        w_pad = jnp.pad(w_qkv, ((0, 0), (0, 0), (0, 0), (0, pad))).reshape(d_model, 3 * n_heads * LANES)
        b_pad = jnp.pad(b_qkv, ((0, 0), (0, 0), (0, pad))).reshape(3 * n_heads * LANES)
        qkv = (jnp.dot(normed_all, w_pad, preferred_element_type=jnp.float32) + b_pad.astype(jnp.float32)).astype(jnp.bfloat16)
        qkv = qkv.reshape(tp * rows, 3, n_heads, LANES).transpose(1, 2, 0, 3)
        context = attention(qkv[0], qkv[1], qkv[2], head_dim)
        context = context[:, :, :head_dim].transpose(1, 0, 2).reshape(tp, rows, n_heads * head_dim)
        received = lax.all_to_all(context, "tp", 0, 0, tiled=True)
        w_out_all = lax.all_gather(w_out.reshape(n_heads * head_dim, d_model), "tp", axis=0, tiled=True)
        ctx = received.transpose(1, 0, 2).reshape(rows, tp * n_heads * head_dim)
        attn = jnp.dot(ctx, w_out_all, preferred_element_type=jnp.float32)
        x1 = (x.astype(jnp.float32) + (attn + b_out.astype(jnp.float32))).astype(jnp.bfloat16)
        h2 = layer_norm(x1, ln2_gain, ln2_bias)
        return mlp(tp, h2, x1, w_up, b_up, w_down, b_down)[None]

    in_layout = (P("dp", "tp", None), P(), P(), P(None, None, "tp", None), P(None, "tp", None), P("tp", None, None), P(), P(), P(), P(None, "tp"), P("tp"), P("tp", None), P())
    return jax.shard_map(device_body, mesh=mesh, in_specs=in_layout, out_specs=P("dp", "tp", None), check_vma=False)
```

```python
import functools
import math

import jax
import jax.numpy as jnp
from jax import lax
from jax.experimental import pallas as pl
from jax.experimental.pallas import tpu as pltpu
from jax.sharding import PartitionSpec as P

LN_EPS = 1e-5
LANES = 128
MESH_IDS = pl.DeviceIdType.MESH


def layer_norm(inputs, gain_vec, shift_vec):
    as_f32 = inputs.astype(jnp.float32)
    row_mean = jnp.mean(as_f32, axis=-1, keepdims=True)
    centered = as_f32 - row_mean
    variance = jnp.mean(centered * centered, axis=-1, keepdims=True)
    return (centered * lax.rsqrt(variance + LN_EPS) * gain_vec + shift_vec).astype(jnp.bfloat16)


def neighbours(tp):
    me = lax.axis_index("tp")
    core = lax.rem(me, 2)
    right = lax.rem(me + 2, tp)
    left = lax.rem(me + tp - 2, tp)
    sibling = me + 1 - 2 * core
    return right, left, sibling


def entry_barrier(peers):
    barrier = pltpu.get_barrier_semaphore()
    for peer in peers:
        pl.semaphore_signal(barrier, inc=1, device_id={"tp": peer}, device_id_type=MESH_IDS)
    pl.semaphore_wait(barrier, len(peers))


def remote(src, dst, send_sem, recv_sem, peer):
    return pltpu.make_async_remote_copy(src_ref=src, dst_ref=dst, send_sem=send_sem, recv_sem=recv_sem,
                                        device_id={"tp": peer}, device_id_type=MESH_IDS)


def attend_kernel(tp, head_dim, x_ref, g_ref, be_ref, w_hbm, b_ref, out_ref,
                  ag, wq, qt_ref, k_ref, vt_ref, pack, got, load_sem, ag_send, ag_recv, push_send, push_recv,
                  ctx_send, ctx_recv):
    n = tp // 2
    half = ag.shape[3]
    rows_own = 2 * half
    d_model = ag.shape[4]
    n_heads = qt_ref.shape[0]
    blk = 2 * rows_own
    me = lax.axis_index("tp")
    core = lax.rem(me, 2)
    chip = me // 2
    right, left, sibling = neighbours(tp)
    ahead = (right, left)

    load = pltpu.make_async_copy(w_hbm, wq, load_sem)
    load.start()
    entry_barrier([lax.rem(me + k, tp) for k in range(1, tp)])

    def forward(s, d):
        return remote(ag.at[s, d, 0], ag.at[s + 1, d, 0], ag_send.at[s, d], ag_recv.at[s + 1, d], ahead[d])

    def push(s, d):
        return remote(ag.at[s, d, 0], ag.at[s, d, 1], push_send.at[s, d], push_recv.at[s, d], sibling)

    ln_rows = 16
    for d in range(2):
        def norm(t, _):
            at = pl.multiple_of(t * ln_rows, ln_rows)
            rows = x_ref[pl.ds(d * half + at, ln_rows), :]
            ag[0, d, 0, pl.ds(at, ln_rows), :] = layer_norm(rows, g_ref[...], be_ref[...])
            return 0

        lax.fori_loop(0, half // ln_rows, norm, 0)
        forward(0, d).start()
        push(0, d).start()
    load.wait()

    def stage(s, _):
        @pl.when(s > 0)
        def _():
            for d in range(2):
                forward(s - 1, d).wait_recv()

                @pl.when(s < n - 1)
                def _():
                    forward(s, d).start()

                push(s, d).start()

        for d in range(2):
            push(s, d).wait_recv()

        source = (lax.rem(chip + n - s, n), lax.rem(chip + s, n))
        starts = [pl.multiple_of((source[d] * 2 + (core if idx == 0 else 1 - core)) * rows_own + d * half, half)
                  for d in range(2) for idx in range(2)]
        width = n_heads * LANES
        for part in range(3):
            cols = slice(part * width, (part + 1) * width)
            acc = jnp.dot(ag[s].reshape(4 * half, d_model), wq[:, cols], preferred_element_type=jnp.float32)
            acc = acc + b_ref[:, cols].astype(jnp.float32)
            for h in range(n_heads):
                for p in range(4):
                    tile = acc[p * half:(p + 1) * half, h * LANES:(h + 1) * LANES]
                    if part == 1:
                        k_ref[h, pl.ds(starts[p], half), :] = tile.astype(jnp.bfloat16)
                    else:
                        (qt_ref if part == 0 else vt_ref)[h, :, pl.ds(starts[p], half)] = tile.T.astype(jnp.bfloat16)
        return 0

    lax.fori_loop(0, n, stage, 0)

    factor = head_dim ** -0.5 * math.log2(math.e)

    def block(qt, j, carry, masked):
        out = []
        rows = pl.ds(pl.multiple_of(j * blk, blk), blk)
        for h in range(n_heads):
            m, l, acc = carry[h]
            s = jnp.dot(k_ref[h, rows, :], qt[h], preferred_element_type=jnp.float32)
            if masked:
                key = lax.broadcasted_iota(jnp.int32, (blk, blk), 0)
                query = lax.broadcasted_iota(jnp.int32, (blk, blk), 1)
                s = jnp.where(query >= key, s, -1e30)
            m_new = jnp.maximum(m, jnp.max(s, axis=0, keepdims=True))
            p = jnp.exp2((s - m_new) * factor)
            alpha = jnp.exp2((m - m_new) * factor)
            l = l * alpha + jnp.sum(p, axis=0, keepdims=True)
            acc = acc * alpha + jnp.dot(vt_ref[h, :head_dim, rows], p.astype(jnp.bfloat16), preferred_element_type=jnp.float32)
            out.append((m_new, l, acc))
        return tuple(out)

    def send_ctx(dest):
        return remote(pack.at[dest], got.at[me], ctx_send.at[dest], ctx_recv.at[me], dest)

    def take_ctx(source):
        return remote(pack.at[source], got.at[source], ctx_send.at[source], ctx_recv.at[source], source)

    def per_chip(t, _):
        step = jnp.where(lax.rem(t, 2) == 1, n // 2 - (t + 1) // 2, n // 2 + t // 2)
        i = lax.rem(chip + step, n)
        cols = pl.ds(pl.multiple_of(i * blk, blk), blk)
        qt = [qt_ref[h, :, cols] for h in range(n_heads)]
        init = tuple((jnp.full((1, blk), -1e30, jnp.float32), jnp.zeros((1, blk), jnp.float32),
                      jnp.zeros((head_dim, blk), jnp.float32)) for _ in range(n_heads))
        carry = block(qt, i, init, True)
        carry = lax.fori_loop(0, i, lambda j, c: block(qt, j, c, False), carry)
        full = jnp.concatenate([acc / l for _, l, acc in carry], axis=0)
        for e in range(2):
            dest = 2 * i + e
            mine = full[:, e * rows_own:(e + 1) * rows_own]
            pack[dest, :rows_own, :] = mine[:LANES].T.astype(jnp.bfloat16)
            tail = jnp.concatenate([mine[LANES:, :half], mine[LANES:, half:]], axis=0)
            pack[dest, rows_own:, :] = tail.T.astype(jnp.bfloat16)

            @pl.when(dest != me)
            def _():
                send_ctx(dest).start()
        return 0

    lax.fori_loop(0, n, per_chip, 0)
    got[me] = pack[me]

    def take(t, _):
        @pl.when(t != me)
        def _():
            take_ctx(t).wait_recv()
        return 0

    lax.fori_loop(0, tp, take, 0)
    rest = LANES // 2
    for c in range(n):
        first, second = got[2 * c], got[2 * c + 1]
        tails = [jnp.concatenate([g[rows_own:, :rest], g[rows_own:, rest:]], axis=0) for g in (first, second)]
        at = c * 3 * LANES
        out_ref[:, at:at + LANES] = first[:rows_own]
        out_ref[:, at + LANES:at + 2 * LANES] = jnp.concatenate([tails[0], second[:rows_own, :rest]], axis=1)
        out_ref[:, at + 2 * LANES:at + 3 * LANES] = jnp.concatenate([second[:rows_own, rest:], tails[1]], axis=1)

    def drain(s, _):
        for d in range(2):
            push(s, d).wait_send()

            @pl.when(s < n - 1)
            def _():
                forward(s, d).wait_send()
        for e in range(2):
            @pl.when(2 * s + e != me)
            def _():
                send_ctx(2 * s + e).wait_send()
        return 0

    lax.fori_loop(0, n, drain, 0)


def attend(tp, x, gain, shift, w_qkv, b_qkv):
    rows, d_model = x.shape
    n_heads, head_dim = w_qkv.shape[2], w_qkv.shape[3]
    assert n_heads == 2 and 2 * n_heads * head_dim == 3 * LANES
    n, half = tp // 2, rows // 2
    seq = tp * rows
    width = 3 * n_heads * LANES
    pad = LANES - head_dim
    w_pad = jnp.pad(w_qkv, ((0, 0), (0, 0), (0, 0), (0, pad))).reshape(d_model, width)
    b_pad = jnp.pad(b_qkv, ((0, 0), (0, 0), (0, pad))).reshape(1, width)
    vmem = pl.BlockSpec(memory_space=pltpu.VMEM)
    hbm = pl.BlockSpec(memory_space=pl.ANY)
    dma = pltpu.SemaphoreType.DMA
    return pl.pallas_call(
        functools.partial(attend_kernel, tp, head_dim),
        out_shape=jax.ShapeDtypeStruct((rows, tp * n_heads * head_dim), jnp.bfloat16),
        in_specs=[vmem, vmem, vmem, hbm, vmem],
        out_specs=vmem,
        scratch_shapes=[
            pltpu.VMEM((n, 2, 2, half, d_model), jnp.bfloat16),
            pltpu.VMEM((d_model, width), jnp.bfloat16),
            pltpu.VMEM((n_heads, LANES, seq), jnp.bfloat16),
            pltpu.VMEM((n_heads, seq, LANES), jnp.bfloat16),
            pltpu.VMEM((n_heads, LANES, seq), jnp.bfloat16),
            pltpu.VMEM((tp, 3 * half, LANES), jnp.bfloat16),
            pltpu.VMEM((tp, 3 * half, LANES), jnp.bfloat16),
            dma,
        ] + [dma((n, 2))] * 4 + [dma((tp,))] * 2,
        compiler_params=pltpu.CompilerParams(collective_id=2, has_side_effects=True, vmem_limit_bytes=67043328),
        cost_estimate=pl.CostEstimate(flops=150 * 10 ** 9, bytes_accessed=2 * d_model * width,
                                      transcendentals=n_heads * seq * seq // 2),
        name="attend",
    )(x, gain.reshape(1, d_model), shift.reshape(1, d_model), w_pad, b_pad)


def mlp_kernel(tp, up_tile, down_tile, h_hbm, x_ref, wu_hbm, bu_ref, wd_hbm, bd_ref, out_ref,
               ag, part, rs, wu, wd, u_ref, load_sem, ag_send, ag_recv, push_send, push_recv,
               part_send, part_recv, rs_send, rs_recv):
    n = tp // 2
    half = ag.shape[3]
    d_model = ag.shape[4]
    ff = wu.shape[1]
    right, left, sibling = neighbours(tp)
    ahead = (right, left)

    loads = [pltpu.make_async_copy(h_hbm.at[pl.ds(d * half, half)], ag.at[0, d, 0], load_sem.at[d]) for d in range(2)]
    loads.append(pltpu.make_async_copy(wu_hbm, wu, load_sem.at[2]))
    loads.append(pltpu.make_async_copy(wd_hbm, wd, load_sem.at[3]))
    for copy in loads:
        copy.start()
    entry_barrier((right, left, sibling))

    def forward(s, d):
        return remote(ag.at[s, d, 0], ag.at[s + 1, d, 0], ag_send.at[s, d], ag_recv.at[s + 1, d], ahead[d])

    def push(s, d):
        return remote(ag.at[s, d, 0], ag.at[s, d, 1], push_send.at[s, d], push_recv.at[s, d], sibling)

    def give(s, d):
        return remote(ag.at[s, d, 1], part.at[s, d], part_send.at[s, d], part_recv.at[s, d], sibling)

    def reduce_send(s, d):
        return remote(part.at[s, d], rs.at[s, d], rs_send.at[s, d], rs_recv.at[s, d], ahead[d])

    for d in range(2):
        loads[d].wait()
        forward(0, d).start()
        push(0, d).start()
    loads[2].wait()
    loads[3].wait()

    def stage(i, _):
        s = lax.rem(i, n)
        last = i == n

        for d in range(2):
            @pl.when(jnp.logical_not(last))
            def _():
                forward(s - 1, d).wait_recv()

                @pl.when(i < n - 1)
                def _():
                    forward(s, d).start()

                push(s, d).start()

        for d in range(2):
            push(s, d).wait_recv()

        def up(t, _):
            cols = pl.ds(pl.multiple_of(t * up_tile, up_tile), up_tile)
            acc = jnp.dot(ag[s].reshape(4 * half, d_model), wu[:, cols], preferred_element_type=jnp.float32)
            u_ref[:, cols] = jax.nn.gelu(acc + bu_ref[:, cols].astype(jnp.float32), approximate=True).astype(jnp.bfloat16)
            return 0

        lax.fori_loop(0, ff // up_tile, up, 0)

        def down_sibling(t, _):
            cols = pl.ds(pl.multiple_of(t * down_tile, down_tile), down_tile)
            lhs = jnp.concatenate([u_ref[pl.ds(half, half), :], u_ref[pl.ds(3 * half, half), :]], axis=0)
            acc = jnp.dot(lhs, wd[:, cols], preferred_element_type=jnp.float32)
            for d in range(2):
                ag[s, d, 1, :, cols] = acc[d * half:(d + 1) * half].astype(jnp.bfloat16)
            return 0

        lax.fori_loop(0, d_model // down_tile, down_sibling, 0)
        for d in range(2):
            give(s, d).start()
        for d in range(2):
            give(s, d).wait_recv()

            @pl.when(i >= 2)
            def _():
                reduce_send(i - 1, d).wait_recv()

        def own_rows(t):
            cols = pl.ds(pl.multiple_of(t * down_tile, down_tile), down_tile)
            lhs = jnp.concatenate([u_ref[pl.ds(0, half), :], u_ref[pl.ds(2 * half, half), :]], axis=0)
            return cols, jnp.dot(lhs, wd[:, cols], preferred_element_type=jnp.float32)

        def add_terms(acc, d, cols, first):
            total = acc[d * half:(d + 1) * half] + part[s, d, :, cols].astype(jnp.float32)
            return total if first else total + rs[i - 1, d, :, cols].astype(jnp.float32)

        def down_first(t, _):
            cols, acc = own_rows(t)
            for d in range(2):
                part[s, d, :, cols] = add_terms(acc, d, cols, True).astype(jnp.bfloat16)
            return 0

        def down_middle(t, _):
            cols, acc = own_rows(t)
            for d in range(2):
                part[s, d, :, cols] = add_terms(acc, d, cols, False).astype(jnp.bfloat16)
            return 0

        def down_last(t, _):
            cols, acc = own_rows(t)
            bias = bd_ref[:, cols].astype(jnp.float32)
            for d in range(2):
                rows = pl.ds(d * half, half)
                total = add_terms(acc, d, cols, False) + bias
                out_ref[rows, cols] = (x_ref[rows, cols].astype(jnp.float32) + total).astype(jnp.bfloat16)
            return 0

        tiles = d_model // down_tile

        @pl.when(i == 1)
        def _():
            lax.fori_loop(0, tiles, down_first, 0)

        @pl.when(jnp.logical_and(i > 1, i < n))
        def _():
            lax.fori_loop(0, tiles, down_middle, 0)

        @pl.when(i < n)
        def _():
            for d in range(2):
                reduce_send(s, d).start()

        @pl.when(last)
        def _():
            lax.fori_loop(0, tiles, down_last, 0)

        return 0

    lax.fori_loop(1, n + 1, stage, 0)

    def drain(s, _):
        for d in range(2):
            push(s, d).wait_send()
            give(s, d).wait_send()

            @pl.when(s < n - 1)
            def _():
                forward(s, d).wait_send()

            @pl.when(s >= 1)
            def _():
                reduce_send(s, d).wait_send()
        return 0

    lax.fori_loop(0, n, drain, 0)


def mlp(tp, h, x, w_up, b_up, w_down, b_down):
    rows, d_model = h.shape
    ff = w_up.shape[1]
    n, half = tp // 2, rows // 2
    up_tile, down_tile = min(256, ff), min(512, d_model)
    vmem = pl.BlockSpec(memory_space=pltpu.VMEM)
    hbm = pl.BlockSpec(memory_space=pl.ANY)
    dma = pltpu.SemaphoreType.DMA
    return pl.pallas_call(
        functools.partial(mlp_kernel, tp, up_tile, down_tile),
        out_shape=jax.ShapeDtypeStruct((rows, d_model), jnp.bfloat16),
        in_specs=[hbm, vmem, hbm, vmem, hbm, vmem],
        out_specs=vmem,
        scratch_shapes=[
            pltpu.VMEM((n, 2, 2, half, d_model), jnp.bfloat16),
            pltpu.VMEM((n, 2, half, d_model), jnp.bfloat16),
            pltpu.VMEM((n, 2, half, d_model), jnp.bfloat16),
            pltpu.VMEM((d_model, ff), jnp.bfloat16),
            pltpu.VMEM((ff, d_model), jnp.bfloat16),
            pltpu.VMEM((4 * half, ff), jnp.bfloat16),
            dma((4,)),
        ] + [dma((n, 2))] * 8,
        compiler_params=pltpu.CompilerParams(collective_id=1, has_side_effects=True, vmem_limit_bytes=67043328),
        cost_estimate=pl.CostEstimate(flops=4 * tp * rows * d_model * ff, bytes_accessed=4 * d_model * ff, transcendentals=tp * rows * ff),
        name="mlp",
    )(h, x, w_up, b_up.reshape(1, ff), w_down, b_down.reshape(1, d_model))


def solution(mesh):
    tp, dp = mesh.shape["tp"], mesh.shape["dp"]

    def device_body(hidden, ln1_gain, ln1_bias, w_qkv, b_qkv, w_out, b_out, ln2_gain, ln2_bias, w_up, b_up, w_down, b_down):
        rows, d_model = hidden.shape[1], hidden.shape[2]
        n_heads, head_dim = w_qkv.shape[2], w_qkv.shape[3]
        x = hidden[0]
        share = n_heads * head_dim // dp
        w_mine = lax.dynamic_slice_in_dim(w_out.reshape(n_heads * head_dim, d_model), lax.axis_index("dp") * share, share, 0)
        w_share = lax.all_gather(w_mine, "tp", axis=0)
        w_all = lax.all_gather(w_share, "dp", axis=0)
        ctx = attend(tp, x, ln1_gain, ln1_bias, w_qkv, b_qkv)
        ctx = ctx.reshape(rows, tp, dp, share)
        attn = jnp.einsum("qtjr,jtre->qe", ctx, w_all, preferred_element_type=jnp.float32)
        x1 = (x.astype(jnp.float32) + (attn + b_out.astype(jnp.float32))).astype(jnp.bfloat16)
        h2 = layer_norm(x1, ln2_gain, ln2_bias)
        return mlp(tp, h2, x1, w_up, b_up, w_down, b_down)[None]

    in_layout = (P("dp", "tp", None), P(), P(), P(None, None, "tp", None), P(None, "tp", None), P("tp", None, None), P(), P(), P(), P(None, "tp"), P("tp"), P("tp", None), P())
    return jax.shard_map(device_body, mesh=mesh, in_specs=in_layout, out_specs=P("dp", "tp", None), check_vma=False)
```
